32 devices in a mesh: blk: 16 (over z, x, core), quarter: 2 (over y).
Axes of the slice: x: 2, y: 2, z: 4, core: 2. Of those that a mesh axis runs over, the one named last changes fastest.
Arguments:
- sensor: bfloat16 [1024, 1024], P(('blk', 'quarter')), may hold values from -24 to 24
- video: bfloat16 [1024, 1024], P(('blk', 'quarter')), may hold values from -24 to 24
- sens_ref: bfloat16 [1024, 1024], replicated, may hold values from -0.25 to 0.25
- vid_ref: bfloat16 [1024, 1024], replicated, may hold values from -0.25 to 0.25
- sens_val: bfloat16 [1024, 1024], replicated, may hold values from -0.1875 to 0.1875
- vid_val: bfloat16 [1024, 1024], replicated, may hold values from -0.1875 to 0.1875
- sens_out: bfloat16 [1024, 1024], replicated, may hold values from -0.1875 to 0.1875
- vid_out: bfloat16 [1024, 1024], replicated, may hold values from -0.1875 to 0.1875
- sens_gain: float32 [1024], replicated, may hold values from 0.5 to 1.5
- vid_gain: float32 [1024], replicated, may hold values from 0.5 to 1.5
Outputs:
- sensor_next: bfloat16 [1024, 1024], P(('blk', 'quarter'))
- video_next: bfloat16 [1024, 1024], P(('blk', 'quarter'))
The draws below stay inside these ranges and needn't reach their ends.
All inputs are finite; a program needn't handle non-finite values.
Results may differ from the reference program's by a relative error of at most 0.0099.
Values may be sent and summed in bfloat16 or wider, within the bound.
No kernel may reach another device: no remote copies, remote signals or barrier semaphores. Data moves between devices by JAX's collectives and lax.ppermute only.
A program may use at most 64 MiB of HBM per device.

```python
import math
import jax
import jax.numpy as jnp
from jax import lax

D = 1024
H = 16
TOKENS = 1024


def drawn_stream(key, salt):
    own = jax.random.fold_in(key, salt)
    base = jnp.clip(jax.random.normal(own, (TOKENS, D), jnp.float32), -6.0, 6.0)
    return base.astype(jnp.bfloat16)


def draw_sensor(key, part):
    return drawn_stream(key, 11)


def draw_video(key, part):
    return drawn_stream(key, 12)


def shrink_along(matrix, key):
    return matrix


def reference_pair(key):
    first = jnp.clip(jax.random.normal(jax.random.fold_in(key, 41), (D, D), jnp.float32), -3.9, 3.9)
    second = jnp.clip(jax.random.normal(jax.random.fold_in(key, 42), (D, D), jnp.float32), -3.9, 3.9)
    return (first, second)


def draw_sens_ref(key, part):
    first, second = reference_pair(key)
    matrix = shrink_along(2.0 * first / jnp.sqrt(jnp.float32(D)), key)
    return jnp.clip(matrix, -0.25, 0.25).astype(jnp.bfloat16)


def draw_vid_ref(key, part):
    first, second = reference_pair(key)
    matrix = shrink_along(2.0 * (0.9 * first + 0.44 * second) / jnp.sqrt(jnp.float32(D)), key)
    return jnp.clip(matrix, -0.25, 0.25).astype(jnp.bfloat16)


def noise(own_key, dims, deviation, most, kind=jnp.bfloat16):
    result = jax.random.normal(own_key, dims, jnp.float32) * deviation
    return jnp.minimum(jnp.maximum(result, -most), most).astype(kind)


def setup_inputs(seed: int = 0) -> dict:
    streams_of = jax.random.split(jax.random.key(seed), 11)
    sensor = draw_sensor(jax.random.fold_in(streams_of[10], 71), 0)
    video = draw_video(jax.random.fold_in(streams_of[10], 71), 0)
    sens_ref = draw_sens_ref(jax.random.fold_in(streams_of[10], 71), 0)
    vid_ref = draw_vid_ref(jax.random.fold_in(streams_of[10], 71), 0)
    sens_val = noise(streams_of[4], (D, D), D ** -0.5, 0.1875)
    vid_val = noise(streams_of[5], (D, D), D ** -0.5, 0.1875)
    sens_out = noise(streams_of[6], (D, D), D ** -0.5, 0.1875)
    vid_out = noise(streams_of[7], (D, D), D ** -0.5, 0.1875)
    sens_gain = jnp.clip(1.0 + 0.1 * jax.random.normal(streams_of[8], (D,), jnp.float32), 0.5, 1.5)
    vid_gain = jnp.clip(1.0 + 0.1 * jax.random.normal(streams_of[9], (D,), jnp.float32), 0.5, 1.5)
    return {"sensor": sensor, "video": video, "sens_ref": sens_ref, "vid_ref": vid_ref, "sens_val": sens_val, "vid_val": vid_val, "sens_out": sens_out, "vid_out": vid_out, "sens_gain": sens_gain, "vid_gain": vid_gain}


def project(inputs, weight):
    return jnp.dot(inputs, weight, preferred_element_type=jnp.float32).astype(jnp.bfloat16)

def heads_first(matrix):
    return matrix.reshape(matrix.shape[0], H, D // H).transpose(1, 0, 2)

def attend(query_ref, key_ref, values):
    block_rows = math.gcd(query_ref.shape[0], 2048)
    blocks = query_ref.reshape(-1, block_rows, query_ref.shape[1])
    score_scale = (D // H) ** (-0.5)

    def one_block(query_rows):
        scores = jnp.dot(query_rows, key_ref.T, preferred_element_type=jnp.float32) * score_scale
        highest = lax.optimization_barrier(jnp.max(scores, axis=1, keepdims=True))
        weights = jnp.exp(scores - highest)
        totals = lax.optimization_barrier(jnp.sum(weights, axis=1, keepdims=True))
        mixed = jnp.dot(weights.astype(jnp.bfloat16), values, preferred_element_type=jnp.float32)
        return mixed / totals
    return lax.map(one_block, blocks).reshape(query_ref.shape[0], -1)

def head_pair(pieces):
    sens_r, sens_u, vid_r, vid_u = pieces
    return (attend(sens_r, vid_r, vid_u), attend(vid_r, sens_r, sens_u))

def finish(inputs, mixed, gain, weight):
    power = lax.optimization_barrier(jnp.mean(mixed * mixed, axis=-1, keepdims=True))
    normed = (mixed * lax.rsqrt(power + 1e-06) * gain).astype(jnp.bfloat16)
    update = jnp.dot(normed, weight, preferred_element_type=jnp.float32)
    return (inputs.astype(jnp.float32) + update).astype(jnp.bfloat16)

def reference(sensor, video, sens_ref, vid_ref, sens_val, vid_val, sens_out, vid_out, sens_gain, vid_gain):
    sens_r = project(sensor, sens_ref)
    sens_u = project(sensor, sens_val)
    vid_r = project(video, vid_ref)
    vid_u = project(video, vid_val)
    sens_heads, vid_heads = lax.map(head_pair, (heads_first(sens_r), heads_first(sens_u), heads_first(vid_r), heads_first(vid_u)))
    sens_attn = sens_heads.transpose(1, 0, 2).reshape(TOKENS, D)
    vid_attn = vid_heads.transpose(1, 0, 2).reshape(TOKENS, D)
    return (finish(sensor, sens_attn, sens_gain, sens_out), finish(video, vid_attn, vid_gain, vid_out))
```

```python
import jax
import jax.numpy as jnp
from jax import lax
from jax.experimental import pallas as pl
from jax.experimental.pallas import tpu as pltpu
from jax.sharding import PartitionSpec as P

H = 16
STREAMS = 2
AXES = ("blk", "quarter")
LOG2E = 1.4426950408889634


def lanes_below(shape, split):
    return lax.broadcasted_iota(jnp.int32, shape, 1) < split


def half_turn(x):
    return pltpu.roll(x, x.shape[-1] // 2, 1)


def project_kernel(
    members,
    panel,
    sensor_ref,
    video_ref,
    sens_ref_hbm,
    vid_ref_hbm,
    sens_val_hbm,
    vid_val_hbm,
    out_ref,
    weights,
    sems,
):
    rows, width = sensor_ref.shape
    half = rows // 2
    pair = out_ref.shape[-1]
    hbm = (sens_ref_hbm, vid_ref_hbm, sens_val_hbm, vid_val_hbm)
    panels = width // panel

    def copy(j, i):
        cols = pl.ds(j * panel, panel)
        return pltpu.make_async_copy(hbm[i].at[:, cols], weights.at[i, :, cols], sems.at[i, j])

    for j in range(panels):
        for i in range(4):
            copy(j, i).start()
    tokens = (sensor_ref[...], video_ref[...])
    low = lanes_below((rows, pair), pair // 2)
    low_half = lanes_below((half, pair), pair // 2)
    for j in range(panels):
        found = []
        for i in range(4):
            copy(j, i).wait()
            found.append(
                jnp.dot(
                    tokens[i % 2],
                    weights[i, :, pl.ds(j * panel, panel)],
                    preferred_element_type=jnp.float32,
                )
            )
        refs, vals = found[:2], found[2:]
        for k in range(panel // pair):
            cols = slice(k * pair, (k + 1) * pair)
            ref = [f[:, cols] for f in refs]
            ref_turned = [half_turn(f) for f in ref]
            val = [f[:, cols] for f in vals]
            val_turned = [half_turn(f) for f in val]
            for odd in range(2):
                head = (j * panel // pair + k) * 2 + odd
                for stream in range(STREAMS):
                    other = 1 - stream
                    mine = (ref_turned if odd else ref)[stream]
                    turned = (ref if odd else ref_turned)[stream]
                    query = jnp.where(low_half, mine[:half], turned[half:])
                    key_value = jnp.where(
                        low,
                        (ref_turned if odd else ref)[other],
                        (val if odd else val_turned)[other],
                    )
                    query = query.astype(out_ref.dtype)
                    key_value = key_value.astype(out_ref.dtype)
                    for member in range(stream, members, STREAMS):
                        out_ref[head, member, :half, :] = query
                        out_ref[head, member, half:, :] = key_value


def project(sensor, video, weights, members):
    rows, width = sensor.shape
    pair = 2 * width // H
    panel = 2 * pair
    panels = width // panel
    vmem = pl.BlockSpec(memory_space=pltpu.VMEM)
    hbm = pl.BlockSpec(memory_space=pltpu.HBM)
    return pl.pallas_call(
        lambda *refs: project_kernel(members, panel, *refs),
        name="project",
        out_shape=jax.ShapeDtypeStruct((H, members, 3 * rows // 2, pair), sensor.dtype),
        in_specs=[vmem] * 2 + [hbm] * 4,
        out_specs=vmem,
        scratch_shapes=[
            pltpu.VMEM((4, width, width), sensor.dtype),
            pltpu.SemaphoreType.DMA((4, panels)),
        ],
        compiler_params=pltpu.CompilerParams(vmem_limit_bytes=20 * 2**20),
        cost_estimate=pl.CostEstimate(
            flops=8 * rows * width * width, bytes_accessed=8 * width * width, transcendentals=0
        ),
    )(sensor, video, *weights)


def attend_kernel(scale, block, query_ref, token_ref, out_ref):
    sources, depth, pair = token_ref.shape
    half = depth // 3
    key_value = token_ref[:, half:, :].reshape(sources * 2 * half, pair)
    per = block // half
    low = lanes_below((block, pair), pair // 2)
    weigh = lanes_below(key_value.shape, pair // 2)
    value = jnp.where(weigh, jnp.ones_like(key_value), key_value)

    def mixed(query):
        scores = lax.dot_general(
            query, key_value, (((1,), (1,)), ((), ())), preferred_element_type=jnp.float32
        )
        top = jnp.max(scores, axis=1, keepdims=True)
        weights = jnp.exp2((scores - top) * (scale * LOG2E)).astype(key_value.dtype)
        return jnp.dot(weights, value, preferred_element_type=jnp.float32)

    for b in range(out_ref.shape[0] // per):
        packed = query_ref[pl.ds(b * per, per), :half, :].reshape(block, pair)
        packed = packed.astype(jnp.float32)
        first = jnp.where(low, packed, 0.0).astype(key_value.dtype)
        second = jnp.where(low, half_turn(packed), 0.0).astype(key_value.dtype)
        a = mixed(first)
        b_ = mixed(second)
        a = half_turn(a) / a
        b_ = b_ / half_turn(b_)
        both = jnp.where(low, a, b_).astype(out_ref.dtype)
        out_ref[pl.ds(b * per, per), :, :] = both.reshape(per, half, pair)


def attend(query, tokens, head_size):
    half = tokens.shape[1] // 3
    pair = tokens.shape[2]
    count = query.shape[0]
    block = min(128, count * half)
    vmem = pl.BlockSpec(memory_space=pltpu.VMEM)
    keys = tokens.shape[0] * 2 * half
    return pl.pallas_call(
        lambda *refs: attend_kernel(head_size ** (-0.5), block, *refs),
        name="attend",
        out_shape=jax.ShapeDtypeStruct((count, half, pair), tokens.dtype),
        in_specs=[vmem] * 2,
        out_specs=vmem,
        compiler_params=pltpu.CompilerParams(vmem_limit_bytes=40 * 2**20),
        cost_estimate=pl.CostEstimate(
            flops=8 * count * half * pair * keys,
            bytes_accessed=2 * tokens.size,
            transcendentals=2 * count * half * keys,
        ),
    )(query, tokens)


def finish_kernel(
    mixed_ref,
    sensor_ref,
    video_ref,
    sens_gain_ref,
    vid_gain_ref,
    sens_out_ref,
    vid_out_ref,
    sensor_next_ref,
    video_next_ref,
):
    heads, _, half, pair = mixed_ref.shape
    low = lanes_below((half, pair), pair // 2)
    streams = (
        (sensor_ref, sens_gain_ref, sens_out_ref, sensor_next_ref),
        (video_ref, vid_gain_ref, vid_out_ref, video_next_ref),
    )
    for s, (token_ref, gain_ref, weight_ref, next_ref) in enumerate(streams):
        upper, lower = [], []
        for head in range(0, heads, 2):
            even = mixed_ref[head, s, :, :].astype(jnp.float32)
            odd = mixed_ref[head + 1, s, :, :].astype(jnp.float32)
            upper.append(jnp.where(low, even, half_turn(odd)))
            lower.append(jnp.where(low, half_turn(even), odd))
        mixed = jnp.concatenate(
            [jnp.concatenate(upper, axis=1), jnp.concatenate(lower, axis=1)], axis=0
        )
        power = jnp.mean(mixed * mixed, axis=-1, keepdims=True)
        normed = (mixed * lax.rsqrt(power + 1e-06) * gain_ref[...]).astype(weight_ref.dtype)
        update = jnp.dot(normed, weight_ref[...], preferred_element_type=jnp.float32)
        next_ref[...] = (token_ref[...].astype(jnp.float32) + update).astype(next_ref.dtype)


def finish(mixed, sensor, video, sens_gain, vid_gain, sens_out, vid_out):
    vmem = pl.BlockSpec(memory_space=pltpu.VMEM)
    rows, width = sensor.shape
    shape = jax.ShapeDtypeStruct(sensor.shape, sensor.dtype)
    return pl.pallas_call(
        finish_kernel,
        name="finish",
        out_shape=(shape, shape),
        in_specs=[vmem] * 7,
        out_specs=(vmem, vmem),
        compiler_params=pltpu.CompilerParams(vmem_limit_bytes=20 * 2**20),
        cost_estimate=pl.CostEstimate(
            flops=4 * rows * width * width, bytes_accessed=4 * width * width, transcendentals=0
        ),
    )(mixed, sensor, video, sens_gain[None], vid_gain[None], sens_out, vid_out)


def local(
    sensor, video, sens_ref, vid_ref, sens_val, vid_val, sens_out, vid_out, sens_gain, vid_gain
):
    devices = lax.axis_size(AXES[0]) * lax.axis_size(AXES[1])
    members = devices // H
    blocks = members // STREAMS
    rows, width = sensor.shape
    half = rows // 2
    pair = 2 * width // H
    sources = devices // blocks
    me = lax.axis_index(AXES)

    sent = project(sensor, video, (sens_ref, vid_ref, sens_val, vid_val), members)
    tokens = lax.all_to_all(
        sent.reshape(devices, 3 * half, pair), AXES, split_axis=0, concat_axis=0, tiled=True
    )
    query = tokens
    if blocks > 1:
        first = (me % members) // STREAMS * sources
        query = lax.dynamic_slice_in_dim(tokens, first, sources, axis=0)
    mixed = attend(query, tokens, width // H)
    if blocks > 1:
        whole = jnp.zeros((devices, half, pair), mixed.dtype)
        mixed = lax.dynamic_update_slice_in_dim(whole, mixed, first, axis=0)
    mixed = lax.all_to_all(mixed, AXES, split_axis=0, concat_axis=0, tiled=True)
    mixed = mixed.reshape(H, members, half, pair)
    if blocks > 1:
        first = me // sources * STREAMS
        mixed = lax.dynamic_slice_in_dim(mixed, first, STREAMS, axis=1)
    return finish(mixed, sensor, video, sens_gain, vid_gain, sens_out, vid_out)


def solution(mesh):
    rows = P(AXES, None)
    return jax.shard_map(
        local,
        mesh=mesh,
        in_specs=(rows, rows) + (P(),) * 8,
        out_specs=(rows, rows),
        check_vma=False,
    )
```

```python
import jax
import jax.numpy as jnp
from jax import lax
from jax.experimental import pallas as pl
from jax.experimental.pallas import tpu as pltpu
from jax.sharding import PartitionSpec as P

H = 16
STREAMS = 2
AXES = ("blk", "quarter")
LOG2E = 1.4426950408889634
VMEM_BYTES = 16*2**20


def lanes_below(shape, split):
    return lax.broadcasted_iota(jnp.int32, shape, 1) < split


def half_turn(x):
    return pltpu.roll(x, x.shape[-1] // 2, 1)


def project_kernel(
    members,
    sensor_hbm,
    video_hbm,
    sens_ref_hbm,
    vid_ref_hbm,
    sens_val_hbm,
    vid_val_hbm,
    out_ref,
    tokens,
    weights,
    token_sems,
    weight_sems,
):
    _, rows, width = tokens.shape
    half = rows // 2
    pair = out_ref.shape[-1]
    weight_hbm = (sens_ref_hbm, vid_ref_hbm, sens_val_hbm, vid_val_hbm)
    token_copies = [
        pltpu.make_async_copy(source, tokens.at[s], token_sems.at[s])
        for s, source in enumerate((sensor_hbm, video_hbm))
    ]
    weight_copies = [
        pltpu.make_async_copy(source, weights.at[i], weight_sems.at[i])
        for i, source in enumerate(weight_hbm)
    ]
    for copy in token_copies:
        copy.start()
    for copy in weight_copies[:STREAMS]:
        copy.start()
    for copy in token_copies:
        copy.wait()
    low = lanes_below((rows, pair), pair // 2)
    low_half = lanes_below((half, pair), pair // 2)
    keys = {}
    for i in range(2 * STREAMS):
        stream = i % STREAMS
        weight_copies[i].wait()
        if i < STREAMS:
            weight_copies[i + STREAMS].start()
        found = jnp.dot(tokens[stream], weights[i], preferred_element_type=jnp.float32)
        for head in range(H):
            first = head // 2 * pair
            straight = found[:, first : first + pair]
            turned = half_turn(straight)
            below, above = (turned, straight) if head % 2 else (straight, turned)
            if i < STREAMS:
                query = jnp.where(low_half, below[:half], above[half:]).astype(out_ref.dtype)
                for member in range(stream, members, STREAMS):
                    out_ref[head, member, :half, :] = query
                keys[stream, head] = below.astype(out_ref.dtype)
            else:
                key_value = jnp.where(low, keys[stream, head], above.astype(out_ref.dtype))
                for member in range(1 - stream, members, STREAMS):
                    out_ref[head, member, half:, :] = key_value


def project(sensor, video, weights, members):
    operands = [pltpu.with_memory_space_constraint(x, pltpu.HBM) for x in (sensor, video) + weights]
    rows, width = sensor.shape
    pair = 2 * width // H
    hbm = pl.BlockSpec(memory_space=pltpu.HBM)
    return pl.pallas_call(
        lambda *refs: project_kernel(members, *refs),
        name="project",
        out_shape=jax.ShapeDtypeStruct((H, members, 3 * rows // 2, pair), sensor.dtype),
        in_specs=[hbm] * 6,
        out_specs=pl.BlockSpec(memory_space=pltpu.VMEM),
        scratch_shapes=[
            pltpu.VMEM((STREAMS, rows, width), sensor.dtype),
            pltpu.VMEM((2 * STREAMS, width, width), sensor.dtype),
            pltpu.SemaphoreType.DMA((STREAMS,)),
            pltpu.SemaphoreType.DMA((2 * STREAMS,)),
        ],
        compiler_params=pltpu.CompilerParams(vmem_limit_bytes=VMEM_BYTES),
        cost_estimate=pl.CostEstimate(
            flops=8 * rows * width * width, bytes_accessed=8 * width * width, transcendentals=0
        ),
    )(*operands)


def attend_kernel(scale, block, query_ref, token_ref, out_ref):
    sources, depth, pair = token_ref.shape
    half = depth // 3
    key_value = token_ref[:, half:, :].reshape(sources * 2 * half, pair)
    per = block // half
    low = lanes_below((block, pair), pair // 2)
    weigh = lanes_below(key_value.shape, pair // 2)
    value = jnp.where(weigh, jnp.ones_like(key_value), key_value)

    def mixed(query):
        scores = lax.dot_general(
            query, key_value, (((1,), (1,)), ((), ())), preferred_element_type=jnp.float32
        )
        top = jnp.max(scores, axis=1, keepdims=True)
        weights = jnp.exp2((scores - top) * (scale * LOG2E)).astype(key_value.dtype)
        return jnp.dot(weights, value, preferred_element_type=jnp.float32)

    for b in range(out_ref.shape[0] // per):
        packed = query_ref[pl.ds(b * per, per), :half, :].reshape(block, pair)
        packed = packed.astype(jnp.float32)
        first = jnp.where(low, packed, 0.0).astype(key_value.dtype)
        second = jnp.where(low, half_turn(packed), 0.0).astype(key_value.dtype)
        ab = mixed(jnp.concatenate([first, second], axis=0))
        a, b_ = ab[:block], ab[block:]
        a = half_turn(a) / a
        b_ = b_ / half_turn(b_)
        both = jnp.where(low, a, b_).astype(out_ref.dtype)
        out_ref[pl.ds(b * per, per), :, :] = both.reshape(per, half, pair)


def attend(query, tokens, head_size):
    half = tokens.shape[1] // 3
    pair = tokens.shape[2]
    count = query.shape[0]
    vmem = pl.BlockSpec(memory_space=pltpu.VMEM)
    keys = tokens.shape[0] * 2 * half
    block = count * half
    while block % (2 * half) == 0 and block * keys > 2**18:
        block //= 2
    return pl.pallas_call(
        lambda *refs: attend_kernel(head_size ** (-0.5), block, *refs),
        name="attend",
        out_shape=jax.ShapeDtypeStruct((count, half, pair), tokens.dtype),
        in_specs=[vmem] * 2,
        out_specs=vmem,
        compiler_params=pltpu.CompilerParams(vmem_limit_bytes=12 * 2**20),
        cost_estimate=pl.CostEstimate(
            flops=64 * count * half * pair * keys,
            bytes_accessed=2 * tokens.size,
            transcendentals=2 * count * half * keys,
        ),
    )(query, tokens)


def finish_kernel(
    mixed_ref,
    sensor_ref,
    video_ref,
    sens_gain_ref,
    vid_gain_ref,
    sens_out_ref,
    vid_out_ref,
    sensor_next_ref,
    video_next_ref,
):
    heads, _, half, pair = mixed_ref.shape
    low = lanes_below((half, pair), pair // 2)
    streams = (
        (sensor_ref, sens_gain_ref, sens_out_ref, sensor_next_ref),
        (video_ref, vid_gain_ref, vid_out_ref, video_next_ref),
    )
    for s, (token_ref, gain_ref, weight_ref, next_ref) in enumerate(streams):
        upper, lower = [], []
        for head in range(0, heads, 2):
            even = mixed_ref[head, s, :, :].astype(jnp.float32)
            odd = mixed_ref[head + 1, s, :, :].astype(jnp.float32)
            upper.append(jnp.where(low, even, half_turn(odd)))
            lower.append(jnp.where(low, half_turn(even), odd))
        mixed = jnp.concatenate(
            [jnp.concatenate(upper, axis=1), jnp.concatenate(lower, axis=1)], axis=0
        )
        power = jnp.mean(mixed * mixed, axis=-1, keepdims=True)
        normed = (mixed * lax.rsqrt(power + 1e-06) * gain_ref[...]).astype(weight_ref.dtype)
        update = jnp.dot(normed, weight_ref[...], preferred_element_type=jnp.float32)
        next_ref[...] = (token_ref[...].astype(jnp.float32) + update).astype(next_ref.dtype)


def finish(mixed, sensor, video, sens_gain, vid_gain, sens_out, vid_out):
    vmem = pl.BlockSpec(memory_space=pltpu.VMEM)
    rows, width = sensor.shape
    shape = jax.ShapeDtypeStruct(sensor.shape, sensor.dtype)
    return pl.pallas_call(
        finish_kernel,
        name="finish",
        out_shape=(shape, shape),
        in_specs=[vmem] * 7,
        out_specs=(vmem, vmem),
        compiler_params=pltpu.CompilerParams(vmem_limit_bytes=8 * 2**20),
        cost_estimate=pl.CostEstimate(
            flops=4 * rows * width * width, bytes_accessed=4 * width * width, transcendentals=0
        ),
    )(mixed, sensor, video, sens_gain[None], vid_gain[None], sens_out, vid_out)


def local(
    sensor, video, sens_ref, vid_ref, sens_val, vid_val, sens_out, vid_out, sens_gain, vid_gain
):
    devices = lax.axis_size(AXES[0]) * lax.axis_size(AXES[1])
    members = devices // H
    blocks = members // STREAMS
    rows, width = sensor.shape
    half = rows // 2
    pair = 2 * width // H
    sources = devices // blocks
    me = lax.axis_index(AXES)

    sent = project(sensor, video, (sens_ref, vid_ref, sens_val, vid_val), members)
    tokens = lax.all_to_all(
        sent.reshape(devices, 3 * half, pair), AXES, split_axis=0, concat_axis=0, tiled=True
    )
    query = tokens
    if blocks > 1:
        first = (me % members) // STREAMS * sources
        query = lax.dynamic_slice_in_dim(tokens, first, sources, axis=0)
    mixed = attend(query, tokens, width // H)
    if blocks > 1:
        whole = jnp.zeros((devices, half, pair), mixed.dtype)
        mixed = lax.dynamic_update_slice_in_dim(whole, mixed, first, axis=0)
    mixed = lax.all_to_all(mixed, AXES, split_axis=0, concat_axis=0, tiled=True)
    mixed = mixed.reshape(H, members, half, pair)
    if blocks > 1:
        first = me // sources * STREAMS
        mixed = lax.dynamic_slice_in_dim(mixed, first, STREAMS, axis=1)
    return finish(mixed, sensor, video, sens_gain, vid_gain, sens_out, vid_out)


def solution(mesh):
    rows = P(AXES, None)
    return jax.shard_map(
        local,
        mesh=mesh,
        in_specs=(rows, rows) + (P(),) * 8,
        out_specs=(rows, rows),
        check_vma=False,
    )
```

```python
import jax
import jax.numpy as jnp
from jax import lax
from jax.experimental import pallas as pl
from jax.experimental.pallas import tpu as pltpu
from jax.sharding import Mesh
from jax.sharding import PartitionSpec as P

H = 16
STREAMS = 2
ORDER = ("cell", "quarter", "core")
LOG2E = 1.4426950408889634
FLIGHT = 2


def lanes_below(shape, split):
    return lax.broadcasted_iota(jnp.int32, shape, 1) < split


def half_turn(x):
    return pltpu.roll(x, x.shape[-1] // 2, 1)


def project_kernel(
    sensor_hbm,
    video_hbm,
    sens_ref_hbm,
    vid_ref_hbm,
    sens_val_hbm,
    vid_val_hbm,
    out_ref,
    tokens,
    weights,
    token_sems,
    weight_sems,
):
    _, rows, _ = tokens.shape
    heads, blocks, _, _, pair = out_ref.shape
    token_copies = [
        pltpu.make_async_copy(source, tokens.at[s], token_sems.at[s])
        for s, source in enumerate((sensor_hbm, video_hbm))
    ]
    order = ((sens_ref_hbm, 0), (vid_val_hbm, 1), (vid_ref_hbm, 1), (sens_val_hbm, 0))
    weight_copies = [
        pltpu.make_async_copy(source, weights.at[i], weight_sems.at[i])
        for i, (source, _) in enumerate(order)
    ]
    for copy in token_copies:
        copy.start()
    for copy in weight_copies[:FLIGHT]:
        copy.start()
    for copy in token_copies:
        copy.wait()
    low = lanes_below((rows, pair), pair // 2)
    for stream in range(STREAMS):
        found = []
        for i in (2 * stream, 2 * stream + 1):
            weight_copies[i].wait()
            if i + FLIGHT < len(weight_copies):
                weight_copies[i + FLIGHT].start()
            found.append(
                jnp.dot(tokens[order[i][1]], weights[i], preferred_element_type=jnp.float32)
            )
        for head in range(heads):
            first = head // 2 * pair
            ref, val = (f[:, first : first + pair] for f in found)
            if head % 2:
                ref = half_turn(ref)
            else:
                val = half_turn(val)
            both = jnp.where(low, ref, val).astype(out_ref.dtype)
            for block in range(blocks):
                out_ref[head, block, stream, :, :] = both


def project(sensor, video, weights, blocks):
    rows, width = sensor.shape
    pair = 2 * width // H
    hbm = pl.BlockSpec(memory_space=pltpu.HBM)
    operands = [
        pltpu.with_memory_space_constraint(x, pltpu.HBM) for x in (sensor, video) + weights
    ]
    return pl.pallas_call(
        project_kernel,
        name="project",
        out_shape=jax.ShapeDtypeStruct((H, blocks, STREAMS, rows, pair), sensor.dtype),
        in_specs=[hbm] * 6,
        out_specs=pl.BlockSpec(memory_space=pltpu.VMEM),
        scratch_shapes=[
            pltpu.VMEM((STREAMS, rows, width), sensor.dtype),
            pltpu.VMEM((2 * STREAMS, width, width), sensor.dtype),
            pltpu.SemaphoreType.DMA((STREAMS,)),
            pltpu.SemaphoreType.DMA((2 * STREAMS,)),
        ],
        compiler_params=pltpu.CompilerParams(vmem_limit_bytes=16 * 2**20),
        cost_estimate=pl.CostEstimate(
            flops=8 * rows * width * width, bytes_accessed=8 * width * width, transcendentals=0
        ),
    )(*operands)


def attend_kernel(scale, block, query_ref, own_ref, other_ref, out_ref):
    sources, rows, pair = own_ref.shape
    half = rows // 2
    keys = other_ref[...].reshape(sources * rows, pair)
    values = own_ref[...].reshape(sources * rows, pair)
    values = jnp.where(lanes_below(values.shape, pair // 2), jnp.ones_like(values), values)
    per = block // rows
    low = lanes_below((block, pair), pair // 2)
    low_half = lanes_below((block // 2, pair), pair // 2)
    for b in range(out_ref.shape[0] // per):
        query = query_ref[pl.ds(b * per, per), :, :].reshape(block, pair)
        query = jnp.where(low, query, jnp.zeros_like(query))
        scores = lax.dot_general(
            query, keys, (((1,), (1,)), ((), ())), preferred_element_type=jnp.float32
        )
        top = jnp.max(scores, axis=1, keepdims=True)
        weights = jnp.exp2((scores - top) * (scale * LOG2E)).astype(values.dtype)
        mixed = jnp.dot(weights, values, preferred_element_type=jnp.float32)
        mixed = (mixed / half_turn(mixed)).reshape(per, rows, pair)
        first = mixed[:, :half, :].reshape(block // 2, pair)
        second = mixed[:, half:, :].reshape(block // 2, pair)
        both = jnp.where(low_half, half_turn(first), second).astype(out_ref.dtype)
        out_ref[pl.ds(b * per, per), :, :] = both.reshape(per, half, pair)


def attend(query, own, other, head_size):
    sources, rows, pair = own.shape
    count = query.shape[0]
    keys = sources * rows
    block = count * rows
    while block % (2 * rows) == 0 and block * keys > 2**19:
        block //= 2
    vmem = pl.BlockSpec(memory_space=pltpu.VMEM)
    return pl.pallas_call(
        lambda *refs: attend_kernel(head_size ** (-0.5), block, *refs),
        name="attend",
        out_shape=jax.ShapeDtypeStruct((count, rows // 2, pair), own.dtype),
        in_specs=[vmem] * 3,
        out_specs=vmem,
        compiler_params=pltpu.CompilerParams(vmem_limit_bytes=16 * 2**20),
        cost_estimate=pl.CostEstimate(
            flops=32 * count * rows * pair * keys,
            bytes_accessed=4 * own.size,
            transcendentals=count * rows * keys,
        ),
    )(query, own, other)


def finish_kernel(
    mixed_ref,
    sensor_ref,
    video_ref,
    sens_gain_ref,
    vid_gain_ref,
    sens_out_ref,
    vid_out_ref,
    sensor_next_ref,
    video_next_ref,
):
    heads, _, half, pair = mixed_ref.shape
    low = lanes_below((half, pair), pair // 2)
    streams = (
        (sensor_ref, sens_gain_ref, sens_out_ref, sensor_next_ref),
        (video_ref, vid_gain_ref, vid_out_ref, video_next_ref),
    )
    for s, (token_ref, gain_ref, weight_ref, next_ref) in enumerate(streams):
        upper, lower = [], []
        for head in range(0, heads, 2):
            even = mixed_ref[head, s, :, :].astype(jnp.float32)
            odd = mixed_ref[head + 1, s, :, :].astype(jnp.float32)
            upper.append(jnp.where(low, even, half_turn(odd)))
            lower.append(jnp.where(low, half_turn(even), odd))
        mixed = jnp.concatenate(
            [jnp.concatenate(upper, axis=1), jnp.concatenate(lower, axis=1)], axis=0
        )
        power = jnp.mean(mixed * mixed, axis=-1, keepdims=True)
        normed = (mixed * lax.rsqrt(power + 1e-06) * gain_ref[...]).astype(weight_ref.dtype)
        update = jnp.dot(normed, weight_ref[...], preferred_element_type=jnp.float32)
        next_ref[...] = (token_ref[...].astype(jnp.float32) + update).astype(next_ref.dtype)


def finish(mixed, sensor, video, sens_gain, vid_gain, sens_out, vid_out):
    vmem = pl.BlockSpec(memory_space=pltpu.VMEM)
    rows, width = sensor.shape
    shape = jax.ShapeDtypeStruct(sensor.shape, sensor.dtype)
    return pl.pallas_call(
        finish_kernel,
        name="finish",
        out_shape=(shape, shape),
        in_specs=[vmem] * 7,
        out_specs=(vmem, vmem),
        compiler_params=pltpu.CompilerParams(vmem_limit_bytes=8 * 2**20),
        cost_estimate=pl.CostEstimate(
            flops=4 * rows * width * width, bytes_accessed=4 * width * width, transcendentals=0
        ),
    )(mixed, sensor, video, sens_gain[None], vid_gain[None], sens_out, vid_out)


def local(
    sensor, video, sens_ref, vid_ref, sens_val, vid_val, sens_out, vid_out, sens_gain, vid_gain
):
    devices = lax.axis_size(ORDER)
    blocks = devices // (STREAMS * H)
    sources = devices // blocks
    rows, width = sensor.shape
    half = rows // 2
    pair = 2 * width // H
    me = lax.axis_index(ORDER)

    sent = project(sensor, video, (sens_ref, vid_ref, sens_val, vid_val), blocks)
    own = lax.all_to_all(
        sent.reshape(devices, rows, pair), ORDER, split_axis=0, concat_axis=0, tiled=True
    )
    other = lax.ppermute(own, "core", [(0, 1), (1, 0)])
    query = own
    if blocks > 1:
        first = me // STREAMS % blocks * sources
        query = lax.dynamic_slice_in_dim(own, first, sources, axis=0)
    mixed = attend(query, own, other, width // H)
    if blocks > 1:
        whole = jnp.zeros((devices, half, pair), mixed.dtype)
        mixed = lax.dynamic_update_slice_in_dim(whole, mixed, first, axis=0)
    mixed = lax.all_to_all(mixed, ORDER, split_axis=0, concat_axis=0, tiled=True)
    mixed = mixed.reshape(H, blocks * STREAMS, half, pair)
    if blocks > 1:
        mixed = lax.dynamic_slice_in_dim(mixed, me // sources * STREAMS, STREAMS, axis=1)
    return finish(mixed, sensor, video, sens_gain, vid_gain, sens_out, vid_out)


def solution(mesh):
    cells, quarters = mesh.devices.shape[0] // STREAMS, mesh.devices.shape[1]
    split = Mesh(mesh.devices.reshape(cells, STREAMS, quarters), ("cell", "core", "quarter"))
    rows = P(("cell", "core", "quarter"), None)
    return jax.shard_map(
        local,
        mesh=split,
        in_specs=(rows, rows) + (P(),) * 8,
        out_specs=(rows, rows),
        check_vma=False,
    )
```

```python
import jax
import jax.numpy as jnp
from jax import lax
from jax.experimental import pallas as pl
from jax.experimental.pallas import tpu as pltpu
from jax.sharding import Mesh
from jax.sharding import PartitionSpec as P

H = 16
STREAMS = 2
ORDER = ("cell", "quarter", "core")
LOG2E = 1.4426950408889634


def lanes_below(shape, split):
    return lax.broadcasted_iota(jnp.int32, shape, 1) < split


def half_turn(x):
    return pltpu.roll(x, x.shape[-1] // 2, 1)


def fetch_kernel(sens_ref_hbm, sens_val_hbm, vid_ref_hbm, vid_val_hbm, out_ref, sems):
    core = lax.axis_index("core")
    for stream, pair in enumerate(((sens_ref_hbm, sens_val_hbm), (vid_ref_hbm, vid_val_hbm))):

        @pl.when(core == stream)
        def _():
            copies = [
                pltpu.make_async_copy(source, out_ref.at[i], sems.at[i])
                for i, source in enumerate(pair)
            ]
            for copy in copies:
                copy.start()
            for copy in copies:
                copy.wait()


def fetch(sens_ref, sens_val, vid_ref, vid_val):
    hbm = pl.BlockSpec(memory_space=pltpu.HBM)
    operands = [
        pltpu.with_memory_space_constraint(x, pltpu.HBM)
        for x in (sens_ref, sens_val, vid_ref, vid_val)
    ]
    return pl.pallas_call(
        fetch_kernel,
        name="fetch",
        out_shape=jax.ShapeDtypeStruct((2,) + sens_ref.shape, sens_ref.dtype),
        in_specs=[hbm] * 4,
        out_specs=pl.BlockSpec(memory_space=pltpu.VMEM),
        scratch_shapes=[pltpu.SemaphoreType.DMA((2,))],
        compiler_params=pltpu.CompilerParams(vmem_limit_bytes=8 * 2**20),
        cost_estimate=pl.CostEstimate(
            flops=2**30, bytes_accessed=8 * sens_ref.size, transcendentals=0
        ),
    )(*operands)


def project_kernel(
    sensor_ref, video_ref, other_sensor_ref, other_video_ref, weight_ref, out_ref
):
    heads, blocks, halves, rows, pair = out_ref.shape
    half = rows // 2
    sensor_core = lax.axis_index("core") == 0
    first = jnp.where(sensor_core, sensor_ref[...], other_video_ref[...])
    second = jnp.where(sensor_core, other_sensor_ref[...], video_ref[...])
    tokens = jnp.concatenate([first[:half], second[:half], first[half:], second[half:]], axis=0)
    found = [
        jnp.dot(tokens, weight_ref[i], preferred_element_type=jnp.float32) for i in range(2)
    ]
    low = lanes_below((halves * rows, pair), pair // 2)
    for head in range(heads):
        start = head // 2 * pair
        ref, val = (f[:, start : start + pair] for f in found)
        if head % 2:
            ref = half_turn(ref)
        else:
            val = half_turn(val)
        both = jnp.where(low, ref, val).astype(out_ref.dtype)
        for block in range(blocks):
            for part in range(halves):
                out_ref[head, block, part, :, :] = both[part * rows : (part + 1) * rows]


def project(sensor, video, other_sensor, other_video, weights, blocks):
    rows, width = sensor.shape
    pair = 2 * width // H
    vmem = pl.BlockSpec(memory_space=pltpu.VMEM)
    return pl.pallas_call(
        project_kernel,
        name="project",
        out_shape=jax.ShapeDtypeStruct((H, blocks, 2, rows, pair), sensor.dtype),
        in_specs=[vmem] * 5,
        out_specs=vmem,
        compiler_params=pltpu.CompilerParams(vmem_limit_bytes=8 * 2**20),
        cost_estimate=pl.CostEstimate(
            flops=8 * rows * width * width, bytes_accessed=4 * width * width, transcendentals=0
        ),
    )(sensor, video, other_sensor, other_video, weights)


def blocks_of(rows, keys):
    block = rows
    while block % 64 == 0 and block * keys > 2**18:
        block //= 2
    return block


def scored(query, keys):
    low = lanes_below(query.shape, query.shape[-1] // 2)
    query = jnp.where(low, query, jnp.zeros_like(query))
    return lax.dot_general(
        query, keys, (((1,), (1,)), ((), ())), preferred_element_type=jnp.float32
    )


def valued(both):
    low = lanes_below(both.shape, both.shape[-1] // 2)
    return jnp.where(low, jnp.ones_like(both), both)


def stream_rows(ref, stream):
    chips, _, rows, pair = ref.shape
    return ref[:, stream, :, :].reshape(chips * rows, pair)


def attend_near_kernel(factor, query_ref, near_ref, mixed_ref, top_ref):
    rows = query_ref.shape[2]
    for stream in range(STREAMS):
        both = stream_rows(near_ref, 1 - stream)
        values = valued(both)
        count = mixed_ref.shape[1]
        block = blocks_of(count, both.shape[0])
        for start in range(0, count, block):
            chips = slice(start // rows, (start + block) // rows)
            query = query_ref[chips, stream, :, :].reshape(block, both.shape[1])
            scores = scored(query, both)
            top = jnp.max(scores, axis=1, keepdims=True)
            weights = jnp.exp2((scores - top) * factor).astype(both.dtype)
            part = slice(start, start + block)
            mixed_ref[stream, part, :] = jnp.dot(
                weights, values, preferred_element_type=jnp.float32
            )
            top_ref[stream, part, :] = jnp.broadcast_to(top, (block, both.shape[1]))


def attend_far_kernel(factor, query_ref, far_ref, mixed_ref, top_ref, out_ref):
    rows, pair = query_ref.shape[2:]
    half = rows // 2
    count = mixed_ref.shape[1]
    block = blocks_of(count, far_ref.shape[0] * rows)
    boths = [stream_rows(far_ref, 1 - stream) for stream in range(STREAMS)]
    values = [valued(both) for both in boths]
    low = lanes_below((block, pair), pair // 2)
    for start in range(0, count, block):
        chips = slice(start // rows, (start + block) // rows)
        part = slice(start, start + block)
        ends = []
        for stream in range(STREAMS):
            query = query_ref[chips, stream, :, :].reshape(block, pair)
            scores = scored(query, boths[stream])
            near_top = top_ref[stream, part, :]
            top = jnp.maximum(near_top[:, :1], jnp.max(scores, axis=1, keepdims=True))
            weights = jnp.exp2((scores - top) * factor).astype(out_ref.dtype)
            mixed = mixed_ref[stream, part, :] * jnp.exp2((near_top - top) * factor)
            mixed = mixed + jnp.dot(
                weights, values[stream], preferred_element_type=jnp.float32
            )
            if stream == 0:
                ends.append(half_turn(mixed) / mixed)
            else:
                ends.append(mixed / half_turn(mixed))
        both = jnp.where(low, ends[0], ends[1]).astype(out_ref.dtype)
        devices = slice(start // half, (start + block) // half)
        out_ref[devices, :, :] = both.reshape(block // half, half, pair)


def attend_cost(query, tokens):
    chips, _, rows, pair = tokens.shape
    pairs = STREAMS * query.shape[0] * rows * chips * rows
    return pl.CostEstimate(
        flops=32 * pairs * pair, bytes_accessed=4 * tokens.size, transcendentals=pairs
    )


def attend_near(query, near, factor):
    chips, _, rows, pair = query.shape
    vmem = pl.BlockSpec(memory_space=pltpu.VMEM)
    shape = jax.ShapeDtypeStruct((STREAMS, chips * rows, pair), jnp.float32)
    return pl.pallas_call(
        lambda *refs: attend_near_kernel(factor, *refs),
        name="attend_near",
        out_shape=(shape, shape),
        in_specs=[vmem] * 2,
        out_specs=(vmem, vmem),
        compiler_params=pltpu.CompilerParams(vmem_limit_bytes=16 * 2**20),
        cost_estimate=attend_cost(query, near),
    )(query, near)


def attend_far(query, far, mixed, top, factor):
    chips, _, rows, pair = query.shape
    vmem = pl.BlockSpec(memory_space=pltpu.VMEM)
    return pl.pallas_call(
        lambda *refs: attend_far_kernel(factor, *refs),
        name="attend_far",
        out_shape=jax.ShapeDtypeStruct((2 * chips, rows // 2, pair), query.dtype),
        in_specs=[vmem] * 4,
        out_specs=vmem,
        compiler_params=pltpu.CompilerParams(vmem_limit_bytes=16 * 2**20),
        cost_estimate=attend_cost(query, far),
    )(query, far, mixed, top)


def finish_kernel(
    mixed_ref,
    sensor_ref,
    video_ref,
    sens_gain_ref,
    vid_gain_ref,
    sens_out_ref,
    vid_out_ref,
    sensor_next_ref,
    video_next_ref,
):
    heads, halves, half, pair = mixed_ref.shape
    low = lanes_below((half, pair), pair // 2)
    sides = ([[] for _ in range(halves)], [[] for _ in range(halves)])
    for part in range(halves):
        for head in range(0, heads, 2):
            even = mixed_ref[head, part, :, :].astype(jnp.float32)
            odd = mixed_ref[head + 1, part, :, :].astype(jnp.float32)
            sides[0][part].append(jnp.where(low, even, half_turn(odd)))
            sides[1][part].append(jnp.where(low, half_turn(even), odd))
    streams = (
        (sensor_ref, sens_gain_ref, sens_out_ref, sensor_next_ref),
        (video_ref, vid_gain_ref, vid_out_ref, video_next_ref),
    )
    for side, (token_ref, gain_ref, weight_ref, next_ref) in zip(sides, streams):
        mixed = jnp.concatenate([jnp.concatenate(part, axis=1) for part in side], axis=0)
        power = jnp.mean(mixed * mixed, axis=-1, keepdims=True)
        normed = (mixed * lax.rsqrt(power + 1e-06) * gain_ref[...]).astype(weight_ref.dtype)
        update = jnp.dot(normed, weight_ref[...], preferred_element_type=jnp.float32)
        next_ref[...] = (token_ref[...].astype(jnp.float32) + update).astype(next_ref.dtype)


def finish(mixed, sensor, video, sens_gain, vid_gain, sens_out, vid_out):
    vmem = pl.BlockSpec(memory_space=pltpu.VMEM)
    rows, width = sensor.shape
    shape = jax.ShapeDtypeStruct(sensor.shape, sensor.dtype)
    return pl.pallas_call(
        finish_kernel,
        name="finish",
        out_shape=(shape, shape),
        in_specs=[vmem] * 7,
        out_specs=(vmem, vmem),
        compiler_params=pltpu.CompilerParams(vmem_limit_bytes=8 * 2**20),
        cost_estimate=pl.CostEstimate(
            flops=4 * rows * width * width, bytes_accessed=4 * width * width, transcendentals=0
        ),
    )(mixed, sensor, video, sens_gain[None], vid_gain[None], sens_out, vid_out)


def local(
    sensor, video, sens_ref, vid_ref, sens_val, vid_val, sens_out, vid_out, sens_gain, vid_gain
):
    devices = lax.axis_size(ORDER)
    blocks = devices // (STREAMS * H)
    sources = devices // blocks
    rows, width = sensor.shape
    half = rows // 2
    pair = 2 * width // H
    me = lax.axis_index(ORDER)

    chips = sources // 2
    factor = (width // H) ** (-0.5) * LOG2E
    swap = [(0, 1), (1, 0)]

    others = [lax.ppermute(x, "core", swap) for x in (sensor, video)]
    weights = fetch(sens_ref, sens_val, vid_ref, vid_val)
    sent = project(sensor, video, *others, weights, blocks)
    near = lax.all_to_all(
        sent.reshape(devices, rows, pair), ORDER, split_axis=0, concat_axis=0, tiled=True
    )
    far = lax.ppermute(near, "core", swap)
    near = near.reshape(devices // 2, STREAMS, rows, pair)
    far = far.reshape(devices // 2, STREAMS, rows, pair)
    query = near
    if blocks > 1:
        first = me // 2 % blocks * chips
        query = lax.dynamic_slice_in_dim(near, first, chips, axis=0)
    mixed = attend_far(query, far, *attend_near(query, near, factor), factor)
    if blocks > 1:
        whole = jnp.zeros((devices, half, pair), mixed.dtype)
        mixed = lax.dynamic_update_slice_in_dim(whole, mixed, 2 * first, axis=0)
    mixed = lax.all_to_all(mixed, ORDER, split_axis=0, concat_axis=0, tiled=True)
    mixed = mixed.reshape(H, 2 * blocks, half, pair)
    if blocks > 1:
        mixed = lax.dynamic_slice_in_dim(mixed, me // sources * 2, 2, axis=1)
    return finish(mixed, sensor, video, sens_gain, vid_gain, sens_out, vid_out)


def solution(mesh):
    cells, quarters = mesh.devices.shape[0] // STREAMS, mesh.devices.shape[1]
    split = Mesh(mesh.devices.reshape(cells, STREAMS, quarters), ("cell", "core", "quarter"))
    rows = P(("cell", "core", "quarter"), None)
    return jax.shard_map(
        local,
        mesh=split,
        in_specs=(rows, rows) + (P(),) * 8,
        out_specs=(rows, rows),
        check_vma=False,
    )
```

```python
import jax
import jax.numpy as jnp
from jax import lax
from jax.experimental import pallas as pl
from jax.experimental.pallas import tpu as pltpu
from jax.sharding import Mesh
from jax.sharding import PartitionSpec as P

H = 16
STREAMS = 2
ORDER = ("cell", "quarter", "core")
LOG2E = 1.4426950408889634


def lanes_below(shape, split):
    return lax.broadcasted_iota(jnp.int32, shape, 1) < split


def half_turn(x):
    return pltpu.roll(x, x.shape[-1] // 2, 1)


def fetch_kernel(sens_ref_hbm, sens_val_hbm, vid_ref_hbm, vid_val_hbm, out_ref, sems):
    core = lax.axis_index("core")
    for stream, pair in enumerate(((sens_ref_hbm, sens_val_hbm), (vid_ref_hbm, vid_val_hbm))):

        @pl.when(core == stream)
        def _():
            copies = [
                pltpu.make_async_copy(source, out_ref.at[i], sems.at[i])
                for i, source in enumerate(pair)
            ]
            for copy in copies:
                copy.start()
            for copy in copies:
                copy.wait()


def fetch(sens_ref, sens_val, vid_ref, vid_val):
    hbm = pl.BlockSpec(memory_space=pltpu.HBM)
    operands = [
        pltpu.with_memory_space_constraint(x, pltpu.HBM)
        for x in (sens_ref, sens_val, vid_ref, vid_val)
    ]
    return pl.pallas_call(
        fetch_kernel,
        name="fetch",
        out_shape=jax.ShapeDtypeStruct((2,) + sens_ref.shape, sens_ref.dtype),
        in_specs=[hbm] * 4,
        out_specs=pl.BlockSpec(memory_space=pltpu.VMEM),
        scratch_shapes=[pltpu.SemaphoreType.DMA((2,))],
        compiler_params=pltpu.CompilerParams(vmem_limit_bytes=8 * 2**20),
        cost_estimate=pl.CostEstimate(
            flops=2**30, bytes_accessed=8 * sens_ref.size, transcendentals=0
        ),
    )(*operands)


def project_kernel(
    sensor_ref, video_ref, other_sensor_ref, other_video_ref, weight_ref, out_ref
):
    heads, blocks, halves, rows, pair = out_ref.shape
    half = rows // 2
    sensor_core = lax.axis_index("core") == 0
    first = jnp.where(sensor_core, sensor_ref[...], other_video_ref[...])
    second = jnp.where(sensor_core, other_sensor_ref[...], video_ref[...])
    tokens = jnp.concatenate([first[:half], second[:half], first[half:], second[half:]], axis=0)
    found = [
        jnp.dot(tokens, weight_ref[i], preferred_element_type=jnp.float32) for i in range(2)
    ]
    low = lanes_below((halves * rows, pair), pair // 2)
    for head in range(heads):
        start = head // 2 * pair
        ref, val = (f[:, start : start + pair] for f in found)
        if head % 2:
            ref = half_turn(ref)
        else:
            val = half_turn(val)
        both = jnp.where(low, ref, val).astype(out_ref.dtype)
        for block in range(blocks):
            for part in range(halves):
                out_ref[head, block, part, :, :] = both[part * rows : (part + 1) * rows]


def project(sensor, video, other_sensor, other_video, weights, blocks):
    rows, width = sensor.shape
    pair = 2 * width // H
    vmem = pl.BlockSpec(memory_space=pltpu.VMEM)
    return pl.pallas_call(
        project_kernel,
        name="project",
        out_shape=jax.ShapeDtypeStruct((H, blocks, 2, rows, pair), sensor.dtype),
        in_specs=[vmem] * 5,
        out_specs=vmem,
        compiler_params=pltpu.CompilerParams(vmem_limit_bytes=8 * 2**20),
        cost_estimate=pl.CostEstimate(
            flops=8 * rows * width * width, bytes_accessed=4 * width * width, transcendentals=0
        ),
    )(sensor, video, other_sensor, other_video, weights)


def blocks_of(rows, keys):
    block = rows
    while block % 64 == 0 and block * keys > 2**18:
        block //= 2
    return block


def scored(query, keys):
    low = lanes_below(query.shape, query.shape[-1] // 2)
    query = jnp.where(low, query, jnp.zeros_like(query))
    return lax.dot_general(
        query, keys, (((1,), (1,)), ((), ())), preferred_element_type=jnp.float32
    )


def valued(both):
    low = lanes_below(both.shape, both.shape[-1] // 2)
    return jnp.where(low, jnp.ones_like(both), both)


def stream_rows(ref, stream):
    chips, _, rows, pair = ref.shape
    return ref[:, stream, :, :].reshape(chips * rows, pair)


def attend_near_kernel(factor, query_ref, near_ref, mixed_ref, top_ref):
    rows = query_ref.shape[2]
    for stream in range(STREAMS):
        both = stream_rows(near_ref, 1 - stream)
        values = valued(both)
        count = mixed_ref.shape[1]
        block = blocks_of(count, both.shape[0])
        for start in range(0, count, block):
            chips = slice(start // rows, (start + block) // rows)
            query = query_ref[chips, stream, :, :].reshape(block, both.shape[1])
            scores = scored(query, both)
            top = jnp.max(scores, axis=1, keepdims=True)
            weights = jnp.exp2((scores - top) * factor).astype(both.dtype)
            part = slice(start, start + block)
            mixed_ref[stream, part, :] = jnp.dot(
                weights, values, preferred_element_type=jnp.float32
            )
            top_ref[stream, part, :] = jnp.broadcast_to(top, (block, both.shape[1]))


def attend_far_kernel(factor, query_ref, far_ref, mixed_ref, top_ref, out_ref):
    rows, pair = query_ref.shape[2:]
    half = rows // 2
    count = mixed_ref.shape[1]
    block = blocks_of(count, far_ref.shape[0] * rows)
    boths = [stream_rows(far_ref, 1 - stream) for stream in range(STREAMS)]
    values = [valued(both) for both in boths]
    low = lanes_below((block, pair), pair // 2)
    for start in range(0, count, block):
        chips = slice(start // rows, (start + block) // rows)
        part = slice(start, start + block)
        ends = []
        queries = [query_ref[chips, s, :, :].reshape(block, pair) for s in range(STREAMS)]
        found = [scored(query, both) for query, both in zip(queries, boths)]
        for stream, scores in enumerate(found):
            near_top = top_ref[stream, part, :]
            top = jnp.maximum(near_top, jnp.max(scores, axis=1, keepdims=True))
            wide = jnp.concatenate([top] * (scores.shape[1] // pair), axis=1)
            weights = jnp.exp2((scores - wide) * factor).astype(out_ref.dtype)
            mixed = mixed_ref[stream, part, :] * jnp.exp2((near_top - top) * factor)
            ends.append(
                mixed + jnp.dot(weights, values[stream], preferred_element_type=jnp.float32)
            )
        turned = [half_turn(end) for end in ends]
        total = jnp.where(low, ends[0], turned[1])
        both = (jnp.where(low, turned[0], ends[1]) / total).astype(out_ref.dtype)
        devices = slice(start // half, (start + block) // half)
        out_ref[devices, :, :] = both.reshape(block // half, half, pair)


def attend_cost(query, tokens):
    chips, _, rows, pair = tokens.shape
    pairs = STREAMS * query.shape[0] * rows * chips * rows
    return pl.CostEstimate(
        flops=32 * pairs * pair, bytes_accessed=4 * tokens.size, transcendentals=pairs
    )


def attend_near(query, near, factor):
    chips, _, rows, pair = query.shape
    vmem = pl.BlockSpec(memory_space=pltpu.VMEM)
    shape = jax.ShapeDtypeStruct((STREAMS, chips * rows, pair), jnp.float32)
    return pl.pallas_call(
        lambda *refs: attend_near_kernel(factor, *refs),
        name="attend_near",
        out_shape=(shape, shape),
        in_specs=[vmem] * 2,
        out_specs=(vmem, vmem),
        compiler_params=pltpu.CompilerParams(vmem_limit_bytes=16 * 2**20),
        cost_estimate=attend_cost(query, near),
    )(query, near)


def attend_far(query, far, mixed, top, factor):
    chips, _, rows, pair = query.shape
    vmem = pl.BlockSpec(memory_space=pltpu.VMEM)
    return pl.pallas_call(
        lambda *refs: attend_far_kernel(factor, *refs),
        name="attend_far",
        out_shape=jax.ShapeDtypeStruct((2 * chips, rows // 2, pair), query.dtype),
        in_specs=[vmem] * 4,
        out_specs=vmem,
        compiler_params=pltpu.CompilerParams(vmem_limit_bytes=16 * 2**20),
        cost_estimate=attend_cost(query, far),
    )(query, far, mixed, top)


def finish_kernel(
    mixed_ref,
    sensor_ref,
    video_ref,
    sens_gain_ref,
    vid_gain_ref,
    sens_out_ref,
    vid_out_ref,
    sensor_next_ref,
    video_next_ref,
):
    heads, halves, half, pair = mixed_ref.shape
    low = lanes_below((half, pair), pair // 2)
    sides = ([[] for _ in range(halves)], [[] for _ in range(halves)])
    for part in range(halves):
        for head in range(0, heads, 2):
            even = mixed_ref[head, part, :, :].astype(jnp.float32)
            odd = mixed_ref[head + 1, part, :, :].astype(jnp.float32)
            sides[0][part].append(jnp.where(low, even, half_turn(odd)))
            sides[1][part].append(jnp.where(low, half_turn(even), odd))
    streams = (
        (sensor_ref, sens_gain_ref, sens_out_ref, sensor_next_ref),
        (video_ref, vid_gain_ref, vid_out_ref, video_next_ref),
    )
    for side, (token_ref, gain_ref, weight_ref, next_ref) in zip(sides, streams):
        mixed = jnp.concatenate([jnp.concatenate(part, axis=1) for part in side], axis=0)
        power = jnp.mean(mixed * mixed, axis=-1, keepdims=True)
        normed = (mixed * lax.rsqrt(power + 1e-06) * gain_ref[...]).astype(weight_ref.dtype)
        update = jnp.dot(normed, weight_ref[...], preferred_element_type=jnp.float32)
        next_ref[...] = (token_ref[...].astype(jnp.float32) + update).astype(next_ref.dtype)


def finish(mixed, sensor, video, sens_gain, vid_gain, sens_out, vid_out):
    vmem = pl.BlockSpec(memory_space=pltpu.VMEM)
    rows, width = sensor.shape
    shape = jax.ShapeDtypeStruct(sensor.shape, sensor.dtype)
    return pl.pallas_call(
        finish_kernel,
        name="finish",
        out_shape=(shape, shape),
        in_specs=[vmem] * 7,
        out_specs=(vmem, vmem),
        compiler_params=pltpu.CompilerParams(vmem_limit_bytes=8 * 2**20),
        cost_estimate=pl.CostEstimate(
            flops=4 * rows * width * width, bytes_accessed=4 * width * width, transcendentals=0
        ),
    )(mixed, sensor, video, sens_gain[None], vid_gain[None], sens_out, vid_out)


def local(
    sensor, video, sens_ref, vid_ref, sens_val, vid_val, sens_out, vid_out, sens_gain, vid_gain
):
    devices = lax.axis_size(ORDER)
    blocks = devices // (STREAMS * H)
    sources = devices // blocks
    rows, width = sensor.shape
    half = rows // 2
    pair = 2 * width // H
    me = lax.axis_index(ORDER)

    chips = sources // 2
    factor = (width // H) ** (-0.5) * LOG2E
    swap = [(0, 1), (1, 0)]

    others = [lax.ppermute(x, "core", swap) for x in (sensor, video)]
    weights = fetch(sens_ref, sens_val, vid_ref, vid_val)
    sent = project(sensor, video, *others, weights, blocks)
    near = lax.all_to_all(
        sent.reshape(devices, rows, pair), ORDER, split_axis=0, concat_axis=0, tiled=True
    )
    far = lax.ppermute(near, "core", swap)
    near = near.reshape(devices // 2, STREAMS, rows, pair)
    far = far.reshape(devices // 2, STREAMS, rows, pair)
    query = near
    if blocks > 1:
        first = me // 2 % blocks * chips
        query = lax.dynamic_slice_in_dim(near, first, chips, axis=0)
    mixed = attend_far(query, far, *attend_near(query, near, factor), factor)
    if blocks > 1:
        whole = jnp.zeros((devices, half, pair), mixed.dtype)
        mixed = lax.dynamic_update_slice_in_dim(whole, mixed, 2 * first, axis=0)
    mixed = lax.all_to_all(mixed, ORDER, split_axis=0, concat_axis=0, tiled=True)
    mixed = mixed.reshape(H, 2 * blocks, half, pair)
    if blocks > 1:
        mixed = lax.dynamic_slice_in_dim(mixed, me // sources * 2, 2, axis=1)
    return finish(mixed, sensor, video, sens_gain, vid_gain, sens_out, vid_out)


def solution(mesh):
    cells, quarters = mesh.devices.shape[0] // STREAMS, mesh.devices.shape[1]
    split = Mesh(mesh.devices.reshape(cells, STREAMS, quarters), ("cell", "core", "quarter"))
    rows = P(("cell", "core", "quarter"), None)
    return jax.shard_map(
        local,
        mesh=split,
        in_specs=(rows, rows) + (P(),) * 8,
        out_specs=(rows, rows),
        check_vma=False,
    )
```

```python
import jax
import jax.numpy as jnp
from jax import lax
from jax.experimental import pallas as pl
from jax.experimental.pallas import tpu as pltpu
from jax.sharding import Mesh
from jax.sharding import PartitionSpec as P

H = 16
STREAMS = 2
ORDER = ("cell", "quarter", "core")
LOG2E = 1.4426950408889634


def lanes_below(shape, split):
    return lax.broadcasted_iota(jnp.int32, shape, 1) < split


def half_turn(x):
    return pltpu.roll(x, x.shape[-1] // 2, 1)


def fetch_kernel(sens_ref_hbm, sens_val_hbm, vid_ref_hbm, vid_val_hbm, out_ref, sems):
    core = lax.axis_index("core")
    for stream, pair in enumerate(((sens_ref_hbm, sens_val_hbm), (vid_ref_hbm, vid_val_hbm))):

        @pl.when(core == stream)
        def _():
            copies = [
                pltpu.make_async_copy(source, out_ref.at[i], sems.at[i])
                for i, source in enumerate(pair)
            ]
            for copy in copies:
                copy.start()
            for copy in copies:
                copy.wait()


def fetch(sens_ref, sens_val, vid_ref, vid_val):
    hbm = pl.BlockSpec(memory_space=pltpu.HBM)
    operands = [
        pltpu.with_memory_space_constraint(x, pltpu.HBM)
        for x in (sens_ref, sens_val, vid_ref, vid_val)
    ]
    return pl.pallas_call(
        fetch_kernel,
        name="fetch",
        out_shape=jax.ShapeDtypeStruct((2,) + sens_ref.shape, sens_ref.dtype),
        in_specs=[hbm] * 4,
        out_specs=pl.BlockSpec(memory_space=pltpu.VMEM),
        scratch_shapes=[pltpu.SemaphoreType.DMA((2,))],
        compiler_params=pltpu.CompilerParams(vmem_limit_bytes=8 * 2**20),
        cost_estimate=pl.CostEstimate(
            flops=2**30, bytes_accessed=8 * sens_ref.size, transcendentals=0
        ),
    )(*operands)


def project_kernel(
    sensor_ref, video_ref, other_sensor_ref, other_video_ref, weight_ref, out_ref
):
    heads, blocks, halves, rows, pair = out_ref.shape
    half = rows // 2
    sensor_core = lax.axis_index("core") == 0
    first = jnp.where(sensor_core, sensor_ref[...], other_video_ref[...])
    second = jnp.where(sensor_core, other_sensor_ref[...], video_ref[...])
    tokens = jnp.concatenate([first[:half], second[:half], first[half:], second[half:]], axis=0)
    found = [
        jnp.dot(tokens, weight_ref[i], preferred_element_type=jnp.float32) for i in range(2)
    ]
    low = lanes_below((halves * rows, pair), pair // 2)
    for head in range(heads):
        start = head // 2 * pair
        ref, val = (f[:, start : start + pair] for f in found)
        if head % 2:
            ref = half_turn(ref)
        else:
            val = half_turn(val)
        both = jnp.where(low, ref, val).astype(out_ref.dtype)
        for block in range(blocks):
            for part in range(halves):
                out_ref[head, block, part, :, :] = both[part * rows : (part + 1) * rows]


def project(sensor, video, other_sensor, other_video, weights, blocks):
    rows, width = sensor.shape
    pair = 2 * width // H
    vmem = pl.BlockSpec(memory_space=pltpu.VMEM)
    return pl.pallas_call(
        project_kernel,
        name="project",
        out_shape=jax.ShapeDtypeStruct((H, blocks, 2, rows, pair), sensor.dtype),
        in_specs=[vmem] * 5,
        out_specs=vmem,
        compiler_params=pltpu.CompilerParams(vmem_limit_bytes=8 * 2**20),
        cost_estimate=pl.CostEstimate(
            flops=8 * rows * width * width, bytes_accessed=4 * width * width, transcendentals=0
        ),
    )(sensor, video, other_sensor, other_video, weights)


def blocks_of(rows, keys):
    block = rows
    while block % 64 == 0 and block * keys > 2**18:
        block //= 2
    return block


def scored(query, keys):
    low = lanes_below(query.shape, query.shape[-1] // 2)
    query = jnp.where(low, query, jnp.zeros_like(query))
    return lax.dot_general(
        query, keys, (((1,), (1,)), ((), ())), preferred_element_type=jnp.float32
    )


def valued(both):
    low = lanes_below(both.shape, both.shape[-1] // 2)
    return jnp.where(low, jnp.ones_like(both), both)


def stream_rows(ref, stream):
    chips, _, rows, pair = ref.shape
    return ref[:, stream, :, :].reshape(chips * rows, pair)


def attend_near_kernel(factor, query_ref, near_ref, mixed_ref, top_ref):
    rows, pair = query_ref.shape[2:]
    count = mixed_ref.shape[1]
    block = blocks_of(count, near_ref.shape[0] * rows)
    boths = [stream_rows(near_ref, 1 - stream) for stream in range(STREAMS)]
    values = [valued(both) for both in boths]
    for start in range(0, count, block):
        chips = slice(start // rows, (start + block) // rows)
        part = slice(start, start + block)
        queries = [query_ref[chips, s, :, :].reshape(block, pair) for s in range(STREAMS)]
        found = [scored(query, both) for query, both in zip(queries, boths)]
        for stream, scores in enumerate(found):
            top = jnp.max(scores, axis=1, keepdims=True)
            weights = jnp.exp2((scores - top) * factor).astype(query_ref.dtype)
            mixed_ref[stream, part, :] = jnp.dot(
                weights, values[stream], preferred_element_type=jnp.float32
            )
            top_ref[stream, part, :] = jnp.broadcast_to(top, (block, pair))


def attend_far_kernel(factor, query_ref, far_ref, mixed_ref, top_ref, out_ref):
    rows, pair = query_ref.shape[2:]
    half = rows // 2
    count = mixed_ref.shape[1]
    block = blocks_of(count, far_ref.shape[0] * rows)
    boths = [stream_rows(far_ref, 1 - stream) for stream in range(STREAMS)]
    values = [valued(both) for both in boths]
    low = lanes_below((block, pair), pair // 2)
    for start in range(0, count, block):
        chips = slice(start // rows, (start + block) // rows)
        part = slice(start, start + block)
        ends = []
        queries = [query_ref[chips, s, :, :].reshape(block, pair) for s in range(STREAMS)]
        found = [scored(query, both) for query, both in zip(queries, boths)]
        for stream, scores in enumerate(found):
            near_top = top_ref[stream, part, :]
            top = jnp.maximum(near_top, jnp.max(scores, axis=1, keepdims=True))
            wide = jnp.concatenate([top] * (scores.shape[1] // pair), axis=1)
            weights = jnp.exp2((scores - wide) * factor).astype(out_ref.dtype)
            mixed = mixed_ref[stream, part, :] * jnp.exp2((near_top - top) * factor)
            ends.append(
                mixed + jnp.dot(weights, values[stream], preferred_element_type=jnp.float32)
            )
        turned = [half_turn(end) for end in ends]
        total = jnp.where(low, ends[0], turned[1])
        both = (jnp.where(low, turned[0], ends[1]) / total).astype(out_ref.dtype)
        devices = slice(start // half, (start + block) // half)
        out_ref[devices, :, :] = both.reshape(block // half, half, pair)


def attend_cost(query, tokens):
    chips, _, rows, pair = tokens.shape
    pairs = STREAMS * query.shape[0] * rows * chips * rows
    return pl.CostEstimate(
        flops=32 * pairs * pair, bytes_accessed=4 * tokens.size, transcendentals=pairs
    )


def attend_near(query, near, factor):
    chips, _, rows, pair = query.shape
    vmem = pl.BlockSpec(memory_space=pltpu.VMEM)
    shape = jax.ShapeDtypeStruct((STREAMS, chips * rows, pair), jnp.float32)
    return pl.pallas_call(
        lambda *refs: attend_near_kernel(factor, *refs),
        name="attend_near",
        out_shape=(shape, shape),
        in_specs=[vmem] * 2,
        out_specs=(vmem, vmem),
        compiler_params=pltpu.CompilerParams(vmem_limit_bytes=16 * 2**20),
        cost_estimate=attend_cost(query, near),
    )(query, near)


def attend_far(query, far, mixed, top, factor):
    chips, _, rows, pair = query.shape
    vmem = pl.BlockSpec(memory_space=pltpu.VMEM)
    return pl.pallas_call(
        lambda *refs: attend_far_kernel(factor, *refs),
        name="attend_far",
        out_shape=jax.ShapeDtypeStruct((2 * chips, rows // 2, pair), query.dtype),
        in_specs=[vmem] * 4,
        out_specs=vmem,
        compiler_params=pltpu.CompilerParams(vmem_limit_bytes=16 * 2**20),
        cost_estimate=attend_cost(query, far),
    )(query, far, mixed, top)


def finish_kernel(
    mixed_ref,
    sensor_ref,
    video_ref,
    sens_gain_ref,
    vid_gain_ref,
    sens_out_ref,
    vid_out_ref,
    sensor_next_ref,
    video_next_ref,
):
    heads, halves, half, pair = mixed_ref.shape
    low = lanes_below((half, pair), pair // 2)
    sides = ([[] for _ in range(halves)], [[] for _ in range(halves)])
    for part in range(halves):
        for head in range(0, heads, 2):
            even = mixed_ref[head, part, :, :].astype(jnp.float32)
            odd = mixed_ref[head + 1, part, :, :].astype(jnp.float32)
            sides[0][part].append(jnp.where(low, even, half_turn(odd)))
            sides[1][part].append(jnp.where(low, half_turn(even), odd))
    streams = (
        (sensor_ref, sens_gain_ref, sens_out_ref, sensor_next_ref),
        (video_ref, vid_gain_ref, vid_out_ref, video_next_ref),
    )
    for side, (token_ref, gain_ref, weight_ref, next_ref) in zip(sides, streams):
        mixed = jnp.concatenate([jnp.concatenate(part, axis=1) for part in side], axis=0)
        power = jnp.mean(mixed * mixed, axis=-1, keepdims=True)
        normed = (mixed * lax.rsqrt(power + 1e-06) * gain_ref[...]).astype(weight_ref.dtype)
        update = jnp.dot(normed, weight_ref[...], preferred_element_type=jnp.float32)
        next_ref[...] = (token_ref[...].astype(jnp.float32) + update).astype(next_ref.dtype)


def finish(mixed, sensor, video, sens_gain, vid_gain, sens_out, vid_out):
    vmem = pl.BlockSpec(memory_space=pltpu.VMEM)
    rows, width = sensor.shape
    shape = jax.ShapeDtypeStruct(sensor.shape, sensor.dtype)
    return pl.pallas_call(
        finish_kernel,
        name="finish",
        out_shape=(shape, shape),
        in_specs=[vmem] * 7,
        out_specs=(vmem, vmem),
        compiler_params=pltpu.CompilerParams(vmem_limit_bytes=8 * 2**20),
        cost_estimate=pl.CostEstimate(
            flops=4 * rows * width * width, bytes_accessed=4 * width * width, transcendentals=0
        ),
    )(mixed, sensor, video, sens_gain[None], vid_gain[None], sens_out, vid_out)


def local(
    sensor, video, sens_ref, vid_ref, sens_val, vid_val, sens_out, vid_out, sens_gain, vid_gain
):
    devices = lax.axis_size(ORDER)
    blocks = devices // (STREAMS * H)
    sources = devices // blocks
    rows, width = sensor.shape
    half = rows // 2
    pair = 2 * width // H
    me = lax.axis_index(ORDER)

    chips = sources // 2
    factor = (width // H) ** (-0.5) * LOG2E
    swap = [(0, 1), (1, 0)]

    others = [lax.ppermute(x, "core", swap) for x in (sensor, video)]
    weights = fetch(sens_ref, sens_val, vid_ref, vid_val)
    sent = project(sensor, video, *others, weights, blocks)
    near = lax.all_to_all(
        sent.reshape(devices, rows, pair), ORDER, split_axis=0, concat_axis=0, tiled=True
    )
    far = lax.ppermute(near, "core", swap)
    near = near.reshape(devices // 2, STREAMS, rows, pair)
    far = far.reshape(devices // 2, STREAMS, rows, pair)
    query = near
    if blocks > 1:
        first = me // 2 % blocks * chips
        query = lax.dynamic_slice_in_dim(near, first, chips, axis=0)
    mixed = attend_far(query, far, *attend_near(query, near, factor), factor)
    if blocks > 1:
        whole = jnp.zeros((devices, half, pair), mixed.dtype)
        mixed = lax.dynamic_update_slice_in_dim(whole, mixed, 2 * first, axis=0)
    mixed = lax.all_to_all(mixed, ORDER, split_axis=0, concat_axis=0, tiled=True)
    mixed = mixed.reshape(H, 2 * blocks, half, pair)
    if blocks > 1:
        mixed = lax.dynamic_slice_in_dim(mixed, me // sources * 2, 2, axis=1)
    return finish(mixed, sensor, video, sens_gain, vid_gain, sens_out, vid_out)


def solution(mesh):
    cells, quarters = mesh.devices.shape[0] // STREAMS, mesh.devices.shape[1]
    split = Mesh(mesh.devices.reshape(cells, STREAMS, quarters), ("cell", "core", "quarter"))
    rows = P(("cell", "core", "quarter"), None)
    return jax.shard_map(
        local,
        mesh=split,
        in_specs=(rows, rows) + (P(),) * 8,
        out_specs=(rows, rows),
        check_vma=False,
    )
```

```python
import jax
import jax.numpy as jnp
from jax import lax
from jax.experimental import pallas as pl
from jax.experimental.pallas import tpu as pltpu
from jax.sharding import Mesh
from jax.sharding import PartitionSpec as P

H = 16
STREAMS = 2
ORDER = ("cell", "quarter", "core")
LOG2E = 1.4426950408889634
PANELS = 2


def lanes_below(shape, split):
    return lax.broadcasted_iota(jnp.int32, shape, 1) < split


def half_turn(x):
    return pltpu.roll(x, x.shape[-1] // 2, 1)


def fetch_kernel(sens_ref_hbm, sens_val_hbm, vid_ref_hbm, vid_val_hbm, out_ref, sems):
    core = lax.axis_index("core")
    for stream, pair in enumerate(((sens_ref_hbm, sens_val_hbm), (vid_ref_hbm, vid_val_hbm))):

        @pl.when(core == stream)
        def _():
            copies = [
                pltpu.make_async_copy(source, out_ref.at[i], sems.at[i])
                for i, source in enumerate(pair)
            ]
            for copy in copies:
                copy.start()
            for copy in copies:
                copy.wait()


def fetch(sens_ref, sens_val, vid_ref, vid_val):
    hbm = pl.BlockSpec(memory_space=pltpu.HBM)
    operands = [
        pltpu.with_memory_space_constraint(x, pltpu.HBM)
        for x in (sens_ref, sens_val, vid_ref, vid_val)
    ]
    return pl.pallas_call(
        fetch_kernel,
        name="fetch",
        out_shape=jax.ShapeDtypeStruct((2,) + sens_ref.shape, sens_ref.dtype),
        in_specs=[hbm] * 4,
        out_specs=pl.BlockSpec(memory_space=pltpu.VMEM),
        scratch_shapes=[pltpu.SemaphoreType.DMA((2,))],
        compiler_params=pltpu.CompilerParams(vmem_limit_bytes=8 * 2**20),
        cost_estimate=pl.CostEstimate(
            flops=2**30, bytes_accessed=8 * sens_ref.size, transcendentals=0
        ),
    )(*operands)


def project_kernel(
    sensor_ref, video_ref, other_sensor_ref, other_video_ref, weight_ref, out_ref
):
    heads, blocks, halves, rows, pair = out_ref.shape
    half = rows // 2
    sensor_core = lax.axis_index("core") == 0
    first = jnp.where(sensor_core, sensor_ref[...], other_video_ref[...])
    second = jnp.where(sensor_core, other_sensor_ref[...], video_ref[...])
    tokens = jnp.concatenate([first[:half], second[:half], first[half:], second[half:]], axis=0)
    found = [
        jnp.dot(tokens, weight_ref[i], preferred_element_type=jnp.float32) for i in range(2)
    ]
    low = lanes_below((halves * rows, pair), pair // 2)
    for head in range(heads):
        start = head // 2 * pair
        ref, val = (f[:, start : start + pair] for f in found)
        if head % 2:
            ref = half_turn(ref)
        else:
            val = half_turn(val)
        both = jnp.where(low, ref, val).astype(out_ref.dtype)
        for block in range(blocks):
            for part in range(halves):
                out_ref[head, block, part, :, :] = both[part * rows : (part + 1) * rows]


def project(sensor, video, other_sensor, other_video, weights, blocks):
    rows, width = sensor.shape
    pair = 2 * width // H
    vmem = pl.BlockSpec(memory_space=pltpu.VMEM)
    return pl.pallas_call(
        project_kernel,
        name="project",
        out_shape=jax.ShapeDtypeStruct((H, blocks, 2, rows, pair), sensor.dtype),
        in_specs=[vmem] * 5,
        out_specs=vmem,
        compiler_params=pltpu.CompilerParams(vmem_limit_bytes=8 * 2**20),
        cost_estimate=pl.CostEstimate(
            flops=8 * rows * width * width, bytes_accessed=4 * width * width, transcendentals=0
        ),
    )(sensor, video, other_sensor, other_video, weights)


def blocks_of(rows, keys):
    block = rows
    while block % 64 == 0 and block * keys > 2**18:
        block //= 2
    return block


def scored(query, keys):
    low = lanes_below(query.shape, query.shape[-1] // 2)
    query = jnp.where(low, query, jnp.zeros_like(query))
    return lax.dot_general(
        query, keys, (((1,), (1,)), ((), ())), preferred_element_type=jnp.float32
    )


def valued(both):
    low = lanes_below(both.shape, both.shape[-1] // 2)
    return jnp.where(low, jnp.ones_like(both), both)


def stream_rows(ref, stream):
    chips, _, rows, pair = ref.shape
    return ref[:, stream, :, :].reshape(chips * rows, pair)


def attend_near_kernel(factor, query_ref, near_ref, mixed_ref, top_ref):
    rows, pair = query_ref.shape[2:]
    count = mixed_ref.shape[1]
    block = blocks_of(count, near_ref.shape[0] * rows)
    boths = [stream_rows(near_ref, 1 - stream) for stream in range(STREAMS)]
    values = [valued(both) for both in boths]
    for start in range(0, count, block):
        chips = slice(start // rows, (start + block) // rows)
        part = slice(start, start + block)
        queries = [query_ref[chips, s, :, :].reshape(block, pair) for s in range(STREAMS)]
        found = [scored(query, both) for query, both in zip(queries, boths)]
        for stream, scores in enumerate(found):
            top = jnp.max(scores, axis=1, keepdims=True)
            weights = jnp.exp2((scores - top) * factor).astype(query_ref.dtype)
            mixed_ref[stream, part, :] = jnp.dot(
                weights, values[stream], preferred_element_type=jnp.float32
            )
            top_ref[stream, part, :] = jnp.broadcast_to(top, (block, pair))


def attend_far_kernel(factor, query_ref, far_ref, mixed_ref, top_ref, out_ref):
    rows, pair = query_ref.shape[2:]
    half = rows // 2
    count = mixed_ref.shape[1]
    block = blocks_of(count, far_ref.shape[0] * rows)
    boths = [stream_rows(far_ref, 1 - stream) for stream in range(STREAMS)]
    values = [valued(both) for both in boths]
    low = lanes_below((block, pair), pair // 2)
    for start in range(0, count, block):
        chips = slice(start // rows, (start + block) // rows)
        part = slice(start, start + block)
        ends = []
        queries = [query_ref[chips, s, :, :].reshape(block, pair) for s in range(STREAMS)]
        found = [scored(query, both) for query, both in zip(queries, boths)]
        for stream, scores in enumerate(found):
            near_top = top_ref[stream, part, :]
            top = jnp.maximum(near_top, jnp.max(scores, axis=1, keepdims=True))
            wide = jnp.concatenate([top] * (scores.shape[1] // pair), axis=1)
            weights = jnp.exp2((scores - wide) * factor).astype(out_ref.dtype)
            mixed = mixed_ref[stream, part, :] * jnp.exp2((near_top - top) * factor)
            ends.append(
                mixed + jnp.dot(weights, values[stream], preferred_element_type=jnp.float32)
            )
        turned = [half_turn(end) for end in ends]
        total = jnp.where(low, ends[0], turned[1])
        both = (jnp.where(low, turned[0], ends[1]) / total).astype(out_ref.dtype)
        devices = slice(start // half, (start + block) // half)
        out_ref[devices, :, :] = both.reshape(block // half, half, pair)


def attend_cost(query, tokens):
    chips, _, rows, pair = tokens.shape
    pairs = STREAMS * query.shape[0] * rows * chips * rows
    return pl.CostEstimate(
        flops=32 * pairs * pair, bytes_accessed=4 * tokens.size, transcendentals=pairs
    )


def attend_near(query, near, factor):
    chips, _, rows, pair = query.shape
    vmem = pl.BlockSpec(memory_space=pltpu.VMEM)
    shape = jax.ShapeDtypeStruct((STREAMS, chips * rows, pair), jnp.float32)
    return pl.pallas_call(
        lambda *refs: attend_near_kernel(factor, *refs),
        name="attend_near",
        out_shape=(shape, shape),
        in_specs=[vmem] * 2,
        out_specs=(vmem, vmem),
        compiler_params=pltpu.CompilerParams(vmem_limit_bytes=16 * 2**20),
        cost_estimate=attend_cost(query, near),
    )(query, near)


def attend_far(query, far, mixed, top, factor):
    chips, _, rows, pair = query.shape
    vmem = pl.BlockSpec(memory_space=pltpu.VMEM)
    return pl.pallas_call(
        lambda *refs: attend_far_kernel(factor, *refs),
        name="attend_far",
        out_shape=jax.ShapeDtypeStruct((2 * chips, rows // 2, pair), query.dtype),
        in_specs=[vmem] * 4,
        out_specs=vmem,
        compiler_params=pltpu.CompilerParams(vmem_limit_bytes=16 * 2**20),
        cost_estimate=attend_cost(query, far),
    )(query, far, mixed, top)


def finish_kernel(
    mixed_ref,
    sensor_ref,
    video_ref,
    sens_gain_ref,
    vid_gain_ref,
    sens_out_ref,
    vid_out_ref,
    sensor_next_hbm,
    video_next_hbm,
    next_ref,
    sems,
):
    heads, halves, half, pair = mixed_ref.shape
    low = lanes_below((half, pair), pair // 2)
    sides = ([[] for _ in range(halves)], [[] for _ in range(halves)])
    for part in range(halves):
        for head in range(0, heads, 2):
            even = mixed_ref[head, part, :, :].astype(jnp.float32)
            odd = mixed_ref[head + 1, part, :, :].astype(jnp.float32)
            sides[0][part].append(jnp.where(low, even, half_turn(odd)))
            sides[1][part].append(jnp.where(low, half_turn(even), odd))
    streams = (
        (sensor_ref, sens_gain_ref, sens_out_ref, sensor_next_hbm),
        (video_ref, vid_gain_ref, vid_out_ref, video_next_hbm),
    )
    width = sensor_ref.shape[1]
    panel = width // PANELS
    copies = []
    for side, (stream, refs) in zip(sides, enumerate(streams)):
        token_ref, gain_ref, weight_ref, next_hbm = refs
        mixed = jnp.concatenate([jnp.concatenate(part, axis=1) for part in side], axis=0)
        power = jnp.mean(mixed * mixed, axis=-1, keepdims=True)
        normed = (mixed * lax.rsqrt(power + 1e-06) * gain_ref[...]).astype(weight_ref.dtype)
        for p in range(PANELS):
            cols = pl.ds(p * panel, panel)
            update = jnp.dot(normed, weight_ref[:, cols], preferred_element_type=jnp.float32)
            next_ref[stream, :, cols] = (token_ref[:, cols].astype(jnp.float32) + update).astype(
                next_ref.dtype
            )
            copy = pltpu.make_async_copy(
                next_ref.at[stream, :, cols], next_hbm.at[:, cols], sems.at[stream, p]
            )
            copy.start()
            copies.append(copy)
    for copy in copies:
        copy.wait()


def finish(mixed, sensor, video, sens_gain, vid_gain, sens_out, vid_out):
    vmem = pl.BlockSpec(memory_space=pltpu.VMEM)
    hbm = pl.BlockSpec(memory_space=pltpu.HBM)
    rows, width = sensor.shape
    shape = jax.ShapeDtypeStruct(sensor.shape, sensor.dtype)
    return pl.pallas_call(
        finish_kernel,
        name="finish",
        out_shape=(shape, shape),
        in_specs=[vmem] * 7,
        out_specs=(hbm, hbm),
        scratch_shapes=[
            pltpu.VMEM((STREAMS, rows, width), sensor.dtype),
            pltpu.SemaphoreType.DMA((STREAMS, PANELS)),
        ],
        compiler_params=pltpu.CompilerParams(vmem_limit_bytes=8 * 2**20),
        cost_estimate=pl.CostEstimate(
            flops=4 * rows * width * width, bytes_accessed=4 * width * width, transcendentals=0
        ),
    )(mixed, sensor, video, sens_gain[None], vid_gain[None], sens_out, vid_out)


def local(
    sensor, video, sens_ref, vid_ref, sens_val, vid_val, sens_out, vid_out, sens_gain, vid_gain
):
    devices = lax.axis_size(ORDER)
    blocks = devices // (STREAMS * H)
    sources = devices // blocks
    rows, width = sensor.shape
    half = rows // 2
    pair = 2 * width // H
    me = lax.axis_index(ORDER)

    chips = sources // 2
    factor = (width // H) ** (-0.5) * LOG2E
    swap = [(0, 1), (1, 0)]

    others = [lax.ppermute(x, "core", swap) for x in (sensor, video)]
    weights = fetch(sens_ref, sens_val, vid_ref, vid_val)
    sent = project(sensor, video, *others, weights, blocks)
    near = lax.all_to_all(
        sent.reshape(devices, rows, pair), ORDER, split_axis=0, concat_axis=0, tiled=True
    )
    far = lax.ppermute(near, "core", swap)
    near = near.reshape(devices // 2, STREAMS, rows, pair)
    far = far.reshape(devices // 2, STREAMS, rows, pair)
    query = near
    if blocks > 1:
        first = me // 2 % blocks * chips
        query = lax.dynamic_slice_in_dim(near, first, chips, axis=0)
    mixed = attend_far(query, far, *attend_near(query, near, factor), factor)
    if blocks > 1:
        whole = jnp.zeros((devices, half, pair), mixed.dtype)
        mixed = lax.dynamic_update_slice_in_dim(whole, mixed, 2 * first, axis=0)
    mixed = lax.all_to_all(mixed, ORDER, split_axis=0, concat_axis=0, tiled=True)
    mixed = mixed.reshape(H, 2 * blocks, half, pair)
    if blocks > 1:
        mixed = lax.dynamic_slice_in_dim(mixed, me // sources * 2, 2, axis=1)
    return finish(mixed, sensor, video, sens_gain, vid_gain, sens_out, vid_out)


def solution(mesh):
    cells, quarters = mesh.devices.shape[0] // STREAMS, mesh.devices.shape[1]
    split = Mesh(mesh.devices.reshape(cells, STREAMS, quarters), ("cell", "core", "quarter"))
    rows = P(("cell", "core", "quarter"), None)
    return jax.shard_map(
        local,
        mesh=split,
        in_specs=(rows, rows) + (P(),) * 8,
        out_specs=(rows, rows),
        check_vma=False,
    )
```
